256 devices in a mesh: vocab: 32 (over z, y), section: 8 (over x, core).
Axes of the slice: x: 4, y: 4, z: 8, core: 2. Of those that a mesh axis runs over, the one named last changes fastest.
Arguments:
- hidden: bfloat16 [512, 8192], P('section', 'vocab'), may hold values from -2 to 2
- targets: int32 [512], replicated, may hold values from 0 to 98303
- out_weight: bfloat16 [98304, 8192], P(('vocab', 'section')), may hold values from -2 to 2
Outputs:
- token_loss: float32 [512], replicated
- weight_grad: bfloat16 [98304, 8192], P(('vocab', 'section'))
- sent_grad: bfloat16 [512, 8192], P('section', 'vocab')
The draws below stay inside these ranges and needn't reach their ends.
All inputs are finite; a program needn't handle non-finite values.
Results may differ from the reference program's by a relative error of at most 0.0033.
Values may be sent and summed in bfloat16 or wider, within the bound.
A program may use at most 128 MiB of HBM per device.

```python
import math
import jax
import jax.numpy as jnp
import numpy as np

D = 8192
TOKENS = 512
VOCAB = 98304
N_SECTION = 8


def weight_row(key, index):
    scale = 13.6 / D ** 0.5
    limit = min(4.0 * scale, 2.0)
    row = scale * jax.random.normal(jax.random.fold_in(key, index), (D,), jnp.float32)
    return jnp.clip(row, -limit, limit)


def weight_rows(key, indices):
    base = jax.random.fold_in(key, 11)
    return jax.vmap(lambda index: weight_row(base, index))(indices)


def draw_out_weight(key, part):
    full = weight_rows(key, jnp.arange(VOCAB, dtype=jnp.int32))
    return full.astype(jnp.bfloat16)


def draw_hidden(key, part):
    inner = jax.random.fold_in(key, 23)
    states = 0.25 * jax.random.normal(inner, (TOKENS, D), jnp.float32)
    return jnp.clip(states, -2.0, 2.0).astype(jnp.bfloat16)


def plant(values, own_key, low, top_value):
    longest = values.shape.index(max(values.shape))
    spots = []
    for shift in (0, 1):
        where = [jax.random.randint(jax.random.fold_in(own_key, axis), (), 0, length) for axis, length in enumerate(values.shape)]
        where[longest] = (where[longest] + shift) % values.shape[longest]
        spots.append(tuple(where))
    return values.at[spots[0]].set(low).at[spots[1]].set(top_value)


def ranked_wide(key, extent, number_of, lean):
    loads = [min(1 << octave, number_of + 1 - (1 << octave)) * (1 << 20) // math.isqrt((1 << octave) ** lean) + 1 for octave in range((number_of + 1).bit_length()) if 1 << octave <= number_of]
    scale = 1 + sum(loads) // (1 << 30)
    grid = np.cumsum(np.array([max(1, weight // scale) for weight in loads]))
    lot = jax.random.randint(jax.random.fold_in(key, 1), extent, 0, int(grid[len(loads) - 1]))
    start = jnp.left_shift(1, jnp.searchsorted(jnp.asarray(grid, jnp.int32), lot, side="right").astype(jnp.int32))
    grade = start - 1 + jax.random.randint(jax.random.fold_in(key, 4), extent, 0, 1 << 30) % jnp.minimum(start, number_of + 1 - start)
    return jax.random.permutation(jax.random.fold_in(key, 2), number_of)[grade].astype(jnp.int32)


def setup_inputs(seed: int = 0) -> dict:
    keys = jax.random.split(jax.random.key(seed), 4)
    hidden = draw_hidden(jax.random.fold_in(keys[3], 71), 0)
    targets = plant(ranked_wide(keys[1], (TOKENS,), VOCAB, 2), jax.random.fold_in(keys[1], 3), 0, VOCAB - 1).astype(jnp.int32)
    out_weight = draw_out_weight(jax.random.fold_in(keys[3], 71), 0)
    return dict(hidden=hidden, targets=targets, out_weight=out_weight)


def reference(hidden, targets, out_weight):
    logits = jnp.dot(hidden, out_weight.T, preferred_element_type=jnp.float32)
    top = jnp.max(logits, axis=1)
    picked = targets[:, None] == jnp.arange(VOCAB, dtype=jnp.int32)[None, :]
    target_logit = jnp.sum(jnp.where(picked, logits, jnp.float32(0.0)), axis=1)
    expd = jnp.exp(logits - top[:, None])
    total = jnp.sum(expd, axis=1)
    token_loss = top + jnp.log(total) - target_logit
    dlogits = (expd / total[:, None] - picked.astype(jnp.float32)).astype(jnp.bfloat16)
    weight_grad = jnp.dot(dlogits.T, hidden, preferred_element_type=jnp.float32).astype(jnp.bfloat16)
    hidden_grad = jnp.dot(dlogits, out_weight, preferred_element_type=jnp.float32)
    sent_grad = jnp.roll(hidden_grad, -(TOKENS // N_SECTION), axis=0).astype(jnp.bfloat16)
    return token_loss, weight_grad, sent_grad
```

```python
import jax
import jax.numpy as jnp
from jax import lax
from jax.experimental import pallas as pl
from jax.experimental.pallas import tpu as pltpu
from jax.sharding import PartitionSpec as P

NZ, NY, NX, NC = 8, 4, 4, 2
D, T, RV = 8192, 512, 384
BC = 48
MESH = pl.DeviceIdType.MESH
F32, BF16 = jnp.float32, jnp.bfloat16
N_SEM = 160


def packed(row):
    return jnp.concatenate([row[:, 128 * k : 128 * (k + 1)] for k in range(4)], axis=0)


def unpacked(block):
    return jnp.concatenate([block[k : k + 1, :] for k in range(4)], axis=1)


def body(hid, tgt, w, loss, wg, dl_out, gat, wv, wo, acc, dlt, stage, rx_c, rx_p, rx_z,
         send_sem, recv_sem, load_sem, own_sem, out_sem):
    v, s = lax.axis_index("vocab"), lax.axis_index("section")
    z, y, x, c = v // NY, lax.rem(v, NY), s // NC, lax.rem(s, NC)
    o = 1 - c

    def dev(z_, y_, x_, c_):
        return (z_ * NY + y_, x_ * NC + c_)

    def zz(k):
        return lax.rem(z + (k + NZ), NZ)

    def yy(k):
        return lax.rem(y + (k + NY), NY)

    def xx(k):
        return lax.rem(x + (k + NX), NX)

    def load_w(k, _):
        own = pltpu.make_async_copy(
            w.at[:, pl.ds(pl.multiple_of(k * 256 + c * 128, 128), 128)], wv.at[k], load_sem.at[0]
        )
        other = pltpu.make_async_copy(
            w.at[:, pl.ds(pl.multiple_of(k * 256 + o * 128, 128), 128)], wo.at[k], load_sem.at[1]
        )
        own.start()
        other.start()
        return 0

    mine = [
        pltpu.make_async_copy(
            hid.at[:, pl.ds(128 * h, 128)], gat.at[h, z, y, x, c], own_sem.at[h]
        )
        for h in range(2)
    ]
    for copy in mine:
        copy.start()
    lax.fori_loop(0, NZ * NY, load_w, 0)

    plane = [(i, j) for i in range(NX) for j in range(NY) if (i, j) != (0, 0)]
    barrier = pltpu.get_barrier_semaphore()
    pl.semaphore_signal(barrier, inc=1, device_id=dev(z, y, x, o), device_id_type=MESH)
    for i, j in plane:
        pl.semaphore_signal(barrier, inc=1, device_id=dev(z, yy(j), xx(i), c), device_id_type=MESH)
    for k in range(1, NZ):
        pl.semaphore_signal(barrier, inc=1, device_id=dev(zz(k), y, x, c), device_id_type=MESH)
    pl.semaphore_wait(barrier, 1 + len(plane) + NZ - 1)
    for copy in mine:
        copy.wait()

    count = [0]
    sends = []

    def slot():
        count[0] += 1
        return count[0] - 1

    def send(ref, device, k):
        copy = pltpu.make_async_remote_copy(
            src_ref=ref, dst_ref=ref, send_sem=send_sem.at[k], recv_sem=recv_sem.at[k],
            device_id=device, device_id_type=MESH,
        )
        copy.start()
        sends.append(copy)

    def arrived(ref, k):
        pltpu.make_async_remote_copy(
            src_ref=ref, dst_ref=ref, send_sem=send_sem.at[k], recv_sem=recv_sem.at[k],
            device_id=dev(z, y, x, o), device_id_type=MESH,
        ).wait_recv()

    passed = []

    def pass_on(view):
        k = slot()
        send(view(c), dev(z, y, x, o), k)
        passed.append((view, k))

    first_z, first_p = [slot() for _ in range(1, NZ)], [slot() for _ in plane]
    for k in range(1, NZ):
        send(gat.at[:, z, y, x, c, 0:BC, :], dev(zz(k), y, x, c), first_z[k - 1])
    for (i, j), k in zip(plane, first_p):
        send(gat.at[:, z, y, x, c, BC:64, :], dev(z, yy(j), xx(i), c), k)

    def b_view(y_, x_, lo, hi):
        return lambda core: gat.at[0, lo:hi, y_, x_, core, 0:BC, :]

    def c_view(y_, x_, lo, hi):
        return lambda core: gat.at[1, lo:hi, y_, x_, core, 0:BC, :]

    def a_view(h, z_):
        return lambda core: gat.at[h, z_, :, :, core, BC:64, :]

    class Ring:
        def __init__(self, view, along):
            self.view, self.along = view, along
            self.k = [slot() for _ in range(4)]

        def to(self, step):
            return dev(z, y, xx(step), c) if self.along == "x" else dev(z, yy(step), x, c)

        def open(self):
            send(self.view(0, 0, NZ)(c), self.to(1), self.k[0])
            send(self.view(0, 0, NZ)(c), self.to(-1), self.k[1])

        def middle(self):
            low, high = self.view(-1, 0, NZ), self.view(1, 0, NZ)
            arrived(low(c), self.k[0])
            send(self.view(-1, 0, 4)(c), self.to(1), self.k[2])
            pass_on(low)
            arrived(high(c), self.k[1])
            send(self.view(1, 4, NZ)(c), self.to(-1), self.k[3])
            pass_on(high)

        def close(self):
            low, high = self.view(-2, 0, 4), self.view(2, 4, NZ)
            arrived(low(c), self.k[2])
            pass_on(low)
            arrived(high(c), self.k[3])
            pass_on(high)

    b_y = Ring(lambda step, lo, hi: b_view(yy(step), x, lo, hi), "y")
    c_x = Ring(lambda step, lo, hi: c_view(y, xx(step), lo, hi), "x")
    b_x = [Ring(lambda step, lo, hi, j=j: b_view(yy(j), xx(step), lo, hi), "x") for j in (0, -1, 1, 2)]
    c_y = [Ring(lambda step, lo, hi, i=i: c_view(yy(step), xx(i), lo, hi), "y") for i in (0, -1, 1, 2)]
    a_up = [[slot() for _ in range(2)] for _ in range(3)] + [[slot()]]
    a_down = [[slot() for _ in range(2)] for _ in range(3)] + [[slot()]]

    for k in range(1, NZ):
        arrived(gat.at[:, zz(-k), y, x, c, 0:BC, :], first_z[k - 1])
    b_y.open()
    c_x.open()
    b_x[0].open()
    c_y[0].open()
    pass_on(lambda core: gat.at[:, :, y, x, core, 0:BC, :])
    for (i, j), k in zip(plane, first_p):
        arrived(gat.at[:, z, yy(-j), xx(-i), c, BC:64, :], k)
    for h in range(2):
        send(a_view(h, z)(c), dev(zz(1), y, x, c), a_up[0][h])
        send(a_view(h, z)(c), dev(zz(-1), y, x, c), a_down[0][h])
    pass_on(lambda core: gat.at[:, z, :, :, core, BC:64, :])

    def a_step(step):
        for h in range(2):
            if h < len(a_up[step - 1]):
                view = a_view(h, zz(-step))
                arrived(view(c), a_up[step - 1][h])
                if step < 3 or (step == 3 and h == 0):
                    send(view(c), dev(zz(1), y, x, c), a_up[step][h])
                pass_on(view)
            lower = h if step < 4 else 1 - h
            if h < len(a_down[step - 1]):
                view = a_view(lower, zz(step))
                arrived(view(c), a_down[step - 1][h])
                if step < 3:
                    send(view(c), dev(zz(-1), y, x, c), a_down[step][h])
                elif step == 3 and h == 1:
                    send(view(c), dev(zz(-1), y, x, c), a_down[step][0])
                pass_on(view)

    b_y.middle()
    b_x[1].open()
    b_x[2].open()
    c_x.middle()
    c_y[1].open()
    c_y[2].open()
    a_step(1)
    b_x[0].middle()
    c_y[0].middle()
    b_y.close()
    b_x[3].open()
    c_x.close()
    c_y[3].open()
    a_step(2)
    b_x[1].middle()
    c_y[1].middle()
    b_x[0].close()
    c_y[0].close()
    b_x[2].middle()
    c_y[2].middle()
    a_step(3)
    b_x[1].close()
    c_y[1].close()
    b_x[3].middle()
    c_y[3].middle()
    b_x[2].close()
    c_y[2].close()
    a_step(4)
    b_x[3].close()
    c_y[3].close()
    for view, k in list(passed):
        arrived(view(o), k)
    pltpu.make_async_copy(wo, wv, load_sem.at[0]).wait()
    pltpu.make_async_copy(wv, wo, load_sem.at[1]).wait()

    acc[...] = jnp.zeros_like(acc)

    def logits_step(k, _):
        left, right = [], []
        for j in range(NY):
            left += [wv[k * NY + j], wo[k * NY + j]]
            right += [gat[c, k, j].reshape(T, 128), gat[o, k, j].reshape(T, 128)]
        acc[...] += lax.dot_general(
            jnp.concatenate(left, axis=1), jnp.concatenate(right, axis=1),
            (((1,), (1,)), ((), ())), preferred_element_type=F32,
        )
        return 0

    lax.fori_loop(0, NZ, logits_step, 0)

    offset = (v * (NX * NC) + s) * RV
    picked = tgt[...] - offset == lax.broadcasted_iota(jnp.int32, (RV, T), 0)
    logits = acc[...]
    hit = jnp.sum(jnp.where(picked, logits, 0.0), axis=0, keepdims=True)
    top = jnp.max(logits, axis=0, keepdims=True)
    total = jnp.sum(jnp.exp(logits - top), axis=0, keepdims=True)
    state = jnp.concatenate([packed(top), packed(total), packed(hit), jnp.zeros((4, 128), F32)], axis=0)

    def merged(blocks):
        tops = [block[0:4] for block in blocks]
        top = tops[0]
        for one in tops[1:]:
            top = jnp.maximum(top, one)
        total, hit = jnp.zeros_like(top), jnp.zeros_like(top)
        for block, one in zip(blocks, tops):
            total = total + block[4:8] * jnp.exp(one - top)
            hit = hit + block[8:12]
        return jnp.concatenate([top, total, hit, jnp.zeros((4, 128), F32)], axis=0)

    def exchanged(state, buf, me, n, peers):
        buf[me] = state
        todo = []
        for device, source, k in peers:
            send(buf.at[me], device, k)
            todo.append((source, k))
        for source, k in todo:
            arrived(buf.at[source], k)
        return merged([buf[k] for k in range(n)])

    state = exchanged(state, rx_c, c, 2, [(dev(z, y, x, o), o, slot())])
    state = exchanged(
        state, rx_p, x * NY + y, NX * NY,
        [(dev(z, yy(j), xx(i), c), xx(-i) * NY + yy(-j), slot()) for i, j in plane],
    )
    state = exchanged(
        state, rx_z, z, NZ, [(dev(zz(k), y, x, c), zz(-k), slot()) for k in range(1, NZ)]
    )
    loss[...] = state[0:4] + jnp.log(state[4:8]) - state[8:12]
    top, total = unpacked(state[0:4]), unpacked(state[4:8])
    dlt[...] = (jnp.exp(acc[...] - top) / total - picked.astype(F32)).astype(BF16)

    for k in range(NZ):
        right = []
        for j in range(NY):
            right += [gat[0, k, j].reshape(T, 128), gat[1, k, j].reshape(T, 128)]
        stage[k] = jnp.dot(
            dlt[...], jnp.concatenate(right, axis=1), preferred_element_type=F32
        ).astype(BF16)
        pltpu.make_async_copy(stage.at[k], wg.at[:, pl.ds(k * 1024, 1024)], out_sem.at[k]).start()
    dl_out[...] = dlt[...]
    for k in range(NZ):
        pltpu.make_async_copy(stage.at[k], wg.at[:, pl.ds(k * 1024, 1024)], out_sem.at[k]).wait()
    for copy in sends:
        copy.wait_send()
    assert count[0] <= N_SEM, count


def forward(hidden, targets, out_weight):
    hbm, vmem = pl.BlockSpec(memory_space=pl.ANY), pl.BlockSpec(memory_space=pltpu.VMEM)
    loss, wg, dlt = pl.pallas_call(
        body,
        out_shape=(
            jax.ShapeDtypeStruct((4, 128), F32),
            jax.ShapeDtypeStruct((RV, D), BF16),
            jax.ShapeDtypeStruct((RV, T), BF16),
        ),
        in_specs=[hbm, vmem, hbm],
        out_specs=(vmem, hbm, vmem),
        scratch_shapes=[
            pltpu.VMEM((2, NZ, NY, NX, NC, 64, 128), BF16),
            pltpu.VMEM((NZ * NY, RV, 128), BF16),
            pltpu.VMEM((NZ * NY, RV, 128), BF16),
            pltpu.VMEM((RV, T), F32),
            pltpu.VMEM((RV, T), BF16),
            pltpu.VMEM((NZ, RV, 1024), BF16),
            pltpu.VMEM((NC, 16, 128), F32),
            pltpu.VMEM((NX * NY, 16, 128), F32),
            pltpu.VMEM((NZ, 16, 128), F32),
            pltpu.SemaphoreType.DMA((N_SEM,)),
            pltpu.SemaphoreType.DMA((N_SEM,)),
            pltpu.SemaphoreType.DMA((2,)),
            pltpu.SemaphoreType.DMA((2,)),
            pltpu.SemaphoreType.DMA((NZ,)),
        ],
        compiler_params=pltpu.CompilerParams(
            collective_id=0, has_side_effects=True, vmem_limit_bytes=60 * 2**20
        ),
    )(hidden, targets.reshape(1, T), out_weight)
    return loss.reshape(T), wg, dlt


def on_device(hidden, targets, out_weight):
    token_loss, weight_grad, dlt = forward(hidden, targets, out_weight)
    partial = lax.dot_general(
        dlt, out_weight, (((0,), (0,)), ((), ())), preferred_element_type=F32
    )
    block = lax.psum_scatter(partial, "section", scatter_dimension=0, tiled=True)
    pieces = jnp.moveaxis(block.reshape(64, NZ * NY, 256), 1, 0)
    owned = lax.all_to_all(pieces, "vocab", split_axis=0, concat_axis=0, tiled=True).sum(axis=0)
    n = NX * NC
    sent = lax.ppermute(owned.astype(BF16), "section", [(k, (k - 1) % n) for k in range(n)])
    return token_loss, weight_grad, sent


def solution(mesh):
    placed = (P("section", "vocab"), P(), P(("vocab", "section"), None))
    return jax.shard_map(
        on_device, mesh=mesh, in_specs=placed,
        out_specs=(P(), P(("vocab", "section"), None), P("section", "vocab")),
        check_vma=False,
    )
```

```python
import jax
import jax.numpy as jnp
from jax import lax
from jax.experimental import pallas as pl
from jax.experimental.pallas import tpu as pltpu
from jax.sharding import PartitionSpec as P

NZ, NY, NX, NC = 8, 4, 4, 2
D, T, RV = 8192, 512, 384
BC = 48
MESH = pl.DeviceIdType.MESH
F32, BF16 = jnp.float32, jnp.bfloat16
N_SEM = 320
WIRE = BF16
A, B, C = slice(0, 32), slice(32, 80), slice(80, 128)
ORDER = (4, 3, -3, 2, -2, 1, -1, 0)


def packed(row):
    return jnp.concatenate([row[:, 128 * k : 128 * (k + 1)] for k in range(4)], axis=0)


def unpacked(block):
    return jnp.concatenate([block[k : k + 1, :] for k in range(4)], axis=1)


def body(hid, tgt, w, loss, wg, sent, gat, wv, wo, acc, dlt, stage, rx_c, rx_p, rx_z, dl, part,
         sb1, rb1, sb2, rb2, sc1, rc1, sc2, rc2, sau, rau, sad, rad, ry1, ry2, rx1, rx2, rz, fa, rp, fin,
         send_sem, recv_sem, load_sem, own_sem, out_sem):
    v, s = lax.axis_index("vocab"), lax.axis_index("section")
    z, y, x, c = v // NY, lax.rem(v, NY), s // NC, lax.rem(s, NC)
    o = 1 - c

    def dev(z_, y_, x_, c_):
        return (z_ * NY + y_, x_ * NC + c_)

    def zz(k):
        return lax.rem(z + (k + NZ), NZ)

    def yy(k):
        return lax.rem(y + (k + NY), NY)

    def xx(k):
        return lax.rem(x + (k + NX), NX)

    def load_w(k, _):
        own = pltpu.make_async_copy(
            w.at[:, pl.ds(pl.multiple_of(k * 256 + c * 128, 128), 128)], wv.at[k, 0:RV], load_sem.at[0]
        )
        other = pltpu.make_async_copy(
            w.at[:, pl.ds(pl.multiple_of(k * 256 + o * 128, 128), 128)], wo.at[k], load_sem.at[1]
        )
        own.start()
        other.start()
        return 0

    mine = [
        pltpu.make_async_copy(
            hid.at[:, pl.ds(128 * h, 128)], gat.at[h, z, y, x, c], own_sem.at[h]
        )
        for h in range(2)
    ]
    for copy in mine:
        copy.start()
    lax.fori_loop(0, NZ * NY, load_w, 0)

    plane = [(i, j) for i in range(NX) for j in range(NY) if (i, j) != (0, 0)]
    barrier = pltpu.get_barrier_semaphore()
    pl.semaphore_signal(barrier, inc=1, device_id=dev(z, y, x, o), device_id_type=MESH)
    for i, j in plane:
        pl.semaphore_signal(barrier, inc=1, device_id=dev(z, yy(j), xx(i), c), device_id_type=MESH)
    for k in range(1, NZ):
        pl.semaphore_signal(barrier, inc=1, device_id=dev(zz(k), y, x, c), device_id_type=MESH)
    pl.semaphore_wait(barrier, 1 + len(plane) + NZ - 1)
    for copy in mine:
        copy.wait()

    count = [0]
    sends = []

    def slot():
        count[0] += 1
        return count[0] - 1

    def send(ref, device, k, to=None):
        copy = pltpu.make_async_remote_copy(
            src_ref=ref, dst_ref=ref if to is None else to, send_sem=send_sem.at[k], recv_sem=recv_sem.at[k],
            device_id=device, device_id_type=MESH,
        )
        copy.start()
        sends.append(copy)

    def arrived(ref, k):
        pltpu.make_async_remote_copy(
            src_ref=ref, dst_ref=ref, send_sem=send_sem.at[k], recv_sem=recv_sem.at[k],
            device_id=dev(z, y, x, o), device_id_type=MESH,
        ).wait_recv()

    passed = []

    def pass_on(view):
        k = slot()
        send(view(c), dev(z, y, x, o), k)
        passed.append((view, k))

    first_z, first_p = [slot() for _ in range(1, NZ)], [slot() for _ in plane]
    for k in range(1, NZ):
        send(gat.at[:, z, y, x, c, 0:BC, :], dev(zz(k), y, x, c), first_z[k - 1])
    for (i, j), k in zip(plane, first_p):
        send(gat.at[:, z, y, x, c, BC:64, :], dev(z, yy(j), xx(i), c), k)

    w_slot = slot()
    pltpu.make_async_copy(wv.at[:, 0:RV, :], wo, load_sem.at[1]).wait()
    send(wo, dev(z, y, x, o), w_slot, wv.at[:, RV : 2 * RV, :])

    def b_view(y_, x_, lo, hi):
        return lambda core: gat.at[0, lo:hi, y_, x_, core, 0:BC, :]

    def c_view(y_, x_, lo, hi):
        return lambda core: gat.at[1, lo:hi, y_, x_, core, 0:BC, :]

    def a_view(h, z_):
        return lambda core: gat.at[h, z_, :, :, core, BC:64, :]

    class Ring:
        def __init__(self, view, along):
            self.view, self.along = view, along
            self.k = [slot() for _ in range(4)]

        def to(self, step):
            return dev(z, y, xx(step), c) if self.along == "x" else dev(z, yy(step), x, c)

        def open(self):
            send(self.view(0, 0, NZ)(c), self.to(1), self.k[0])
            send(self.view(0, 0, NZ)(c), self.to(-1), self.k[1])

        def middle(self):
            low, high = self.view(-1, 0, NZ), self.view(1, 0, NZ)
            arrived(low(c), self.k[0])
            send(self.view(-1, 0, 4)(c), self.to(1), self.k[2])
            pass_on(low)
            arrived(high(c), self.k[1])
            send(self.view(1, 4, NZ)(c), self.to(-1), self.k[3])
            pass_on(high)

        def close(self):
            low, high = self.view(-2, 0, 4), self.view(2, 4, NZ)
            arrived(low(c), self.k[2])
            pass_on(low)
            arrived(high(c), self.k[3])
            pass_on(high)

    b_y = Ring(lambda step, lo, hi: b_view(yy(step), x, lo, hi), "y")
    c_x = Ring(lambda step, lo, hi: c_view(y, xx(step), lo, hi), "x")
    b_x = [Ring(lambda step, lo, hi, j=j: b_view(yy(j), xx(step), lo, hi), "x") for j in (0, -1, 1, 2)]
    c_y = [Ring(lambda step, lo, hi, i=i: c_view(yy(step), xx(i), lo, hi), "y") for i in (0, -1, 1, 2)]
    a_up = [[slot() for _ in range(2)] for _ in range(3)] + [[slot()]]
    a_down = [[slot() for _ in range(2)] for _ in range(3)] + [[slot()]]

    for k in range(1, NZ):
        arrived(gat.at[:, zz(-k), y, x, c, 0:BC, :], first_z[k - 1])
    b_y.open()
    c_x.open()
    b_x[0].open()
    c_y[0].open()
    pass_on(lambda core: gat.at[:, :, y, x, core, 0:BC, :])
    for (i, j), k in zip(plane, first_p):
        arrived(gat.at[:, z, yy(-j), xx(-i), c, BC:64, :], k)
    for h in range(2):
        send(a_view(h, z)(c), dev(zz(1), y, x, c), a_up[0][h])
        send(a_view(h, z)(c), dev(zz(-1), y, x, c), a_down[0][h])
    pass_on(lambda core: gat.at[:, z, :, :, core, BC:64, :])

    def a_step(step):
        for h in range(2):
            if h < len(a_up[step - 1]):
                view = a_view(h, zz(-step))
                arrived(view(c), a_up[step - 1][h])
                if step < 3 or (step == 3 and h == 0):
                    send(view(c), dev(zz(1), y, x, c), a_up[step][h])
                pass_on(view)
            lower = h if step < 4 else 1 - h
            if h < len(a_down[step - 1]):
                view = a_view(lower, zz(step))
                arrived(view(c), a_down[step - 1][h])
                if step < 3:
                    send(view(c), dev(zz(-1), y, x, c), a_down[step][h])
                elif step == 3 and h == 1:
                    send(view(c), dev(zz(-1), y, x, c), a_down[step][0])
                pass_on(view)

    b_y.middle()
    b_x[1].open()
    b_x[2].open()
    c_x.middle()
    c_y[1].open()
    c_y[2].open()
    a_step(1)
    b_x[0].middle()
    c_y[0].middle()
    b_y.close()
    b_x[3].open()
    c_x.close()
    c_y[3].open()
    a_step(2)
    b_x[1].middle()
    c_y[1].middle()
    b_x[0].close()
    c_y[0].close()
    b_x[2].middle()
    c_y[2].middle()
    a_step(3)
    b_x[1].close()
    c_y[1].close()
    b_x[3].middle()
    c_y[3].middle()
    b_x[2].close()
    c_y[2].close()
    a_step(4)
    b_x[3].close()
    c_y[3].close()
    for view, k in list(passed):
        arrived(view(o), k)
    arrived(wv.at[:, RV : 2 * RV, :], w_slot)
    pltpu.make_async_copy(wo, wv.at[:, 0:RV, :], load_sem.at[0]).wait()

    acc[...] = jnp.zeros_like(acc)

    def logits_step(k, _):
        left, right = [], []
        for j in range(NY):
            left += [wv[k * NY + j, 0:RV], wo[k * NY + j]]
            right += [gat[c, k, j].reshape(T, 128), gat[o, k, j].reshape(T, 128)]
        acc[...] += lax.dot_general(
            jnp.concatenate(left, axis=1), jnp.concatenate(right, axis=1),
            (((1,), (1,)), ((), ())), preferred_element_type=F32,
        )
        return 0

    lax.fori_loop(0, NZ, logits_step, 0)

    offset = (v * (NX * NC) + s) * RV
    picked = tgt[...] - offset == lax.broadcasted_iota(jnp.int32, (RV, T), 0)
    logits = acc[...]
    hit = jnp.sum(jnp.where(picked, logits, 0.0), axis=0, keepdims=True)
    top = jnp.max(logits, axis=0, keepdims=True)
    total = jnp.sum(jnp.exp(logits - top), axis=0, keepdims=True)
    state = jnp.concatenate([packed(top), packed(total), packed(hit), jnp.zeros((4, 128), F32)], axis=0)

    def merged(blocks):
        tops = [block[0:4] for block in blocks]
        top = tops[0]
        for one in tops[1:]:
            top = jnp.maximum(top, one)
        total, hit = jnp.zeros_like(top), jnp.zeros_like(top)
        for block, one in zip(blocks, tops):
            total = total + block[4:8] * jnp.exp(one - top)
            hit = hit + block[8:12]
        return jnp.concatenate([top, total, hit, jnp.zeros((4, 128), F32)], axis=0)

    def exchanged(state, buf, me, n, peers):
        buf[me] = state
        todo = []
        for device, source, k in peers:
            send(buf.at[me], device, k)
            todo.append((source, k))
        for source, k in todo:
            arrived(buf.at[source], k)
        return merged([buf[k] for k in range(n)])

    state = exchanged(state, rx_c, c, 2, [(dev(z, y, x, o), o, slot())])
    state = exchanged(
        state, rx_p, x * NY + y, NX * NY,
        [(dev(z, yy(j), xx(i), c), xx(-i) * NY + yy(-j), slot()) for i, j in plane],
    )
    state = exchanged(
        state, rx_z, z, NZ, [(dev(zz(k), y, x, c), zz(-k), slot()) for k in range(1, NZ)]
    )
    loss[...] = state[0:4] + jnp.log(state[4:8]) - state[8:12]
    top, total = unpacked(state[0:4]), unpacked(state[4:8])
    dlt[...] = (jnp.exp(acc[...] - top) / total - picked.astype(F32)).astype(BF16)

    own = jnp.transpose(dlt[...])
    dl[:, 0:RV] = jnp.concatenate([own[64:T], own[0:64]], axis=0)
    dl_slot = slot()
    send(dl.at[:, 0:RV], dev(z, y, x, o), dl_slot, dl.at[:, RV : 2 * RV])

    def weight_step(k):
        right = []
        for j in range(NY):
            right += [gat[0, k, j].reshape(T, 128), gat[1, k, j].reshape(T, 128)]
        stage[k] = jnp.dot(
            dlt[...], jnp.concatenate(right, axis=1), preferred_element_type=F32
        ).astype(BF16)
        pltpu.make_async_copy(stage.at[k], wg.at[:, pl.ds(k * 1024, 1024)], out_sem.at[k]).start()

    def hidden_step(i):
        zd = zz(ORDER[i])
        right = jnp.concatenate([wv[zd * NY + j] for j in range(NY)], axis=1)
        res = jnp.dot(dl[...], right, preferred_element_type=F32)
        for j in range(NY):
            part[i, j] = res[:, 128 * j : 128 * (j + 1)].reshape(NX, 128, 128)

    class Heavy:
        def __init__(self, unit, along, s1, r1, s2, r2):
            self.unit, self.along = unit, along
            self.s1, self.r1, self.s2, self.r2 = s1, r1, s2, r2
            self.k = [[slot() for _ in range(4)] for _ in range(NZ)]

        def to(self, step):
            return dev(z, y, xx(step), c) if self.along == "x" else dev(z, yy(step), x, c)

        def first(self, i):
            self.s1[i] = self.unit(i, 2).astype(WIRE)
            k = self.k[i]
            send(self.s1.at[i, 0:2], self.to(1), k[0], self.r1.at[i, 0:2])
            send(self.s1.at[i, 2:4], self.to(-1), k[1], self.r1.at[i, 2:4])

        def second(self, i):
            k = self.k[i]
            for d, lo, hi in ((0, 0, 2), (1, 2, 4)):
                step = 1 - 2 * d
                arrived(self.r1.at[i, lo:hi], k[d])
                mine = self.unit(i, step)
                self.s2[i, d] = mine.astype(WIRE)
                self.s2[i, d, lo:hi] = (mine[lo:hi] + self.r1[i, lo:hi].astype(F32)).astype(WIRE)
                send(self.s2.at[i, d], self.to(step), k[2 + d], self.r2.at[i, d])

        def third(self, i):
            for d in range(2):
                arrived(self.r2.at[i, d], self.k[i][2 + d])
            return self.unit(i, 0) + self.r2[i, 0].astype(F32) + self.r2[i, 1].astype(F32)

    hb = Heavy(lambda i, step: part[i, :, xx(step), B, :], "x", sb1, rb1, sb2, rb2)
    hc = Heavy(lambda i, step: part[i, yy(step), :, C, :], "y", sc1, rc1, sc2, rc2)

    def thirds(i):
        part[i, :, x, B, :] = hb.third(i)
        part[i, y, :, C, :] = hc.third(i)

    class Light:
        def __init__(self, at, along, r1, r2):
            self.at, self.along, self.r1, self.r2 = at, along, r1, r2
            self.k = [[slot() for _ in range(4)] for _ in range(2)]

        def to(self, step):
            return dev(z, y, xx(step), c) if self.along == "x" else dev(z, yy(step), x, c)

        def first(self, g):
            lo, k = 4 * g, self.k[g]
            send(part.at[lo : lo + 2, *self.at(2)], self.to(1), k[0], self.r1.at[g, 0:2])
            send(part.at[lo + 2 : lo + 4, *self.at(2)], self.to(-1), k[1], self.r1.at[g, 2:4])

        def second(self, g):
            lo, k = 4 * g, self.k[g]
            for d in range(2):
                step, h = 1 - 2 * d, 2 * d
                arrived(self.r1.at[g, h : h + 2], k[d])
                where = (slice(lo + h, lo + h + 2), *self.at(step))
                part[where] = part[where] + self.r1[g, h : h + 2]
                send(part.at[lo : lo + 4, *self.at(step)], self.to(step), k[2 + d], self.r2.at[g, d])

        def third(self, g):
            for d in range(2):
                arrived(self.r2.at[g, d], self.k[g][2 + d])
            where = (slice(4 * g, 4 * g + 4), *self.at(0))
            part[where] = part[where] + self.r2[g, 0] + self.r2[g, 1]

    lb = Light(lambda step: (yy(step), x, B), "y", ry1, ry2)
    lc = Light(lambda step: (y, xx(step), C), "x", rx1, rx2)

    k_up = {(off, h): slot() for off in (4, 3, 2, 1) for h in range(2)}
    k_down = {(off, h): slot() for off in (4, 3, 2, 1) for h in range(2)}

    def a_send(up, off, h):
        i = ORDER.index(off if up or off == 4 else -off)
        src, dst, ks, step = (sau, rau, k_up, 1) if up else (sad, rad, k_down, -1)
        rows = slice(2 * h, 2 * h + 2)
        value = part[i, rows, :, A, :]
        if off < 3 or (off == 3 and h == (0 if up else 1)):
            arrived(dst.at[off, rows], ks[off + 1, h])
            value = value + dst[off, rows].astype(F32)
        src[off - 1, rows] = value.astype(WIRE)
        send(src.at[off - 1, rows], dev(zz(step), y, x, c), ks[off, h], dst.at[off - 1, rows])

    k_plane = [slot() for _ in plane]
    k_z = [slot() for _ in range(NZ - 1)]

    def a_plane():
        for h in range(2):
            arrived(rau.at[0, 2 * h : 2 * h + 2], k_up[1, h])
            arrived(rad.at[0, 2 * h : 2 * h + 2], k_down[1, h])
        fa[...] = part[NZ - 1, :, :, A, :] + rau[0].astype(F32) + rad[0].astype(F32)
        for q, (i, j) in enumerate(plane):
            send(fa.at[yy(j), xx(i)], dev(z, yy(j), xx(i), c), k_plane[q], rp.at[q])

    def z_send(i):
        send(part.at[i, y, x, 32:128, :], dev(zz(ORDER[i]), y, x, c), k_z[i], rz.at[i])

    weight_step(0)
    weight_step(1)
    arrived(dl.at[:, RV : 2 * RV], dl_slot)
    for i in range(NZ):
        hidden_step(i)
        if i == 0:
            a_send(True, 4, 0)
            a_send(False, 4, 1)
        hb.first(i)
        hc.first(i)
        if i == 1:
            a_send(True, 3, 1)
        if i == 2:
            a_send(False, 3, 0)
        if i == 4:
            a_send(True, 3, 0)
            a_send(False, 3, 1)
        if i >= 4:
            hb.second(i - 4)
            hc.second(i - 4)
        if i == 6:
            for h in range(2):
                a_send(True, 2, h)
                a_send(False, 2, h)
    hb.second(4)
    hc.second(4)
    weight_step(2)
    for h in range(2):
        a_send(True, 1, h)
        a_send(False, 1, h)
    hb.second(5)
    hc.second(5)
    weight_step(3)
    for i in range(4):
        thirds(i)
    lb.first(0)
    lc.first(0)
    hb.second(6)
    hc.second(6)
    hb.second(7)
    hc.second(7)
    weight_step(4)
    a_plane()
    lb.second(0)
    lc.second(0)
    weight_step(5)
    for i in range(4, 8):
        thirds(i)
    lb.first(1)
    lc.first(1)
    weight_step(6)
    lb.third(0)
    lc.third(0)
    for i in range(4):
        z_send(i)
    weight_step(7)
    lb.second(1)
    lc.second(1)
    for q in range(len(plane)):
        arrived(rp.at[q], k_plane[q])
    a_rows = fa[y, x]
    for q in range(len(plane)):
        a_rows = a_rows + rp[q]
    fa[y, x] = a_rows
    lb.third(1)
    lc.third(1)
    for i in range(4, 7):
        z_send(i)
    bc_rows = part[NZ - 1, y, x, 32:128, :]
    for i in range(NZ - 1):
        arrived(rz.at[i], k_z[i])
        bc_rows = bc_rows + rz[i]
    rows = jnp.concatenate([fa[y, x], bc_rows], axis=0).astype(BF16)
    fin_slot = slot()
    fin[0, 0] = rows[0:64]
    fin[0, 1] = rows[64:128]
    send(fin.at[0, o], dev(z, y, x, o), fin_slot, fin.at[1, 0])
    arrived(fin.at[1, 0], fin_slot)
    for core in range(2):

        @pl.when(c == core)
        def _():
            sent[:, 128 * core : 128 * (core + 1)] = fin[0, core]
            sent[:, 128 * (1 - core) : 128 * (2 - core)] = fin[1, 0]

    for k in range(NZ):
        pltpu.make_async_copy(stage.at[k], wg.at[:, pl.ds(k * 1024, 1024)], out_sem.at[k]).wait()
    for copy in sends:
        copy.wait_send()
    assert count[0] <= N_SEM, count


def on_device(hidden, targets, out_weight):
    hbm, vmem = pl.BlockSpec(memory_space=pl.ANY), pl.BlockSpec(memory_space=pltpu.VMEM)
    heavy = [
        pltpu.VMEM((NZ, 4, BC, 128), WIRE),
        pltpu.VMEM((NZ, 4, BC, 128), WIRE),
        pltpu.VMEM((NZ, 2, 4, BC, 128), WIRE),
        pltpu.VMEM((NZ, 2, 4, BC, 128), WIRE),
    ]
    loss, weight_grad, sent = pl.pallas_call(
        body,
        out_shape=(
            jax.ShapeDtypeStruct((4, 128), F32),
            jax.ShapeDtypeStruct((RV, D), BF16),
            jax.ShapeDtypeStruct((64, 256), BF16),
        ),
        in_specs=[hbm, vmem, hbm],
        out_specs=(vmem, hbm, vmem),
        scratch_shapes=[
            pltpu.VMEM((2, NZ, NY, NX, NC, 64, 128), BF16),
            pltpu.VMEM((NZ * NY, 2 * RV, 128), BF16),
            pltpu.VMEM((NZ * NY, RV, 128), BF16),
            pltpu.VMEM((RV, T), F32),
            pltpu.VMEM((RV, T), BF16),
            pltpu.VMEM((NZ, RV, 1024), BF16),
            pltpu.VMEM((NC, 16, 128), F32),
            pltpu.VMEM((NX * NY, 16, 128), F32),
            pltpu.VMEM((NZ, 16, 128), F32),
            pltpu.VMEM((T, 2 * RV), BF16),
            pltpu.VMEM((NZ, NY, NX, 128, 128), F32),
            *heavy,
            *heavy,
            pltpu.VMEM((4, NY, NX, 32, 128), WIRE),
            pltpu.VMEM((4, NY, NX, 32, 128), WIRE),
            pltpu.VMEM((4, NY, NX, 32, 128), WIRE),
            pltpu.VMEM((4, NY, NX, 32, 128), WIRE),
            pltpu.VMEM((2, 4, BC, 128), F32),
            pltpu.VMEM((2, 2, 4, BC, 128), F32),
            pltpu.VMEM((2, 4, BC, 128), F32),
            pltpu.VMEM((2, 2, 4, BC, 128), F32),
            pltpu.VMEM((NZ - 1, 96, 128), F32),
            pltpu.VMEM((NY, NX, 32, 128), F32),
            pltpu.VMEM((NX * NY - 1, 32, 128), F32),
            pltpu.VMEM((2, 2, 64, 128), BF16),
            pltpu.SemaphoreType.DMA((N_SEM,)),
            pltpu.SemaphoreType.DMA((N_SEM,)),
            pltpu.SemaphoreType.DMA((2,)),
            pltpu.SemaphoreType.DMA((2,)),
            pltpu.SemaphoreType.DMA((NZ,)),
        ],
        compiler_params=pltpu.CompilerParams(
            collective_id=0, has_side_effects=True, vmem_limit_bytes=62 * 2**20
        ),
    )(hidden, targets.reshape(1, T), out_weight)
    return loss.reshape(T), weight_grad, sent


def solution(mesh):
    placed = (P("section", "vocab"), P(), P(("vocab", "section"), None))
    return jax.shard_map(
        on_device, mesh=mesh, in_specs=placed,
        out_specs=(P(), P(("vocab", "section"), None), P("section", "vocab")),
        check_vma=False,
    )
```

```python
import jax
import jax.numpy as jnp
from jax import lax
from jax.experimental import pallas as pl
from jax.experimental.pallas import tpu as pltpu
from jax.sharding import PartitionSpec as P

NZ, NY, NX, NC = 8, 4, 4, 2
D, T, RV = 8192, 512, 384
MESH = pl.DeviceIdType.MESH
F32, BF16 = jnp.float32, jnp.bfloat16
N_SEM = 400
WIRE = BF16
B, C = slice(0, 64), slice(64, 128)
NEAR = (0, -1, 1, -2, 2, -3, 3, 4)
ORDER = (4, 3, -3, 2, -2, 1, -1, 0)


def packed(row):
    return jnp.concatenate([row[:, 128 * k : 128 * (k + 1)] for k in range(4)], axis=0)


def unpacked(block):
    return jnp.concatenate([block[k : k + 1, :] for k in range(4)], axis=1)


def body(hid, tgt, w, loss, wg, sent, gat, wv, wo, acc, acc_o, dlt, rx_c, rx_p, rx_z, dl, part,
         sb1, rb1, sb2, rb2, sc1, rc1, sc2, rc2, qs, zb, rzb, rzf, fz, rf,
         send_sem, recv_sem, load_sem, own_sem):
    v, s = lax.axis_index("vocab"), lax.axis_index("section")
    z, y, x, c = v // NY, lax.rem(v, NY), s // NC, lax.rem(s, NC)
    o = 1 - c

    def dev(z_, y_, x_, c_):
        return (z_ * NY + y_, x_ * NC + c_)

    def zz(k):
        return lax.rem(z + (k + NZ), NZ)

    def yy(k):
        return lax.rem(y + (k + NY), NY)

    def xx(k):
        return lax.rem(x + (k + NX), NX)

    def load_w(k, _):
        own = pltpu.make_async_copy(
            w.at[:, pl.ds(pl.multiple_of(k * 256 + c * 128, 128), 128)], wv.at[k, 0:RV], load_sem.at[0]
        )
        other = pltpu.make_async_copy(
            w.at[:, pl.ds(pl.multiple_of(k * 256 + o * 128, 128), 128)], wo.at[k], load_sem.at[1]
        )
        own.start()
        other.start()
        return 0

    mine = [
        pltpu.make_async_copy(
            hid.at[:, pl.ds(128 * h, 128)], gat.at[h, z, y, x, c], own_sem.at[h]
        )
        for h in range(2)
    ]
    for copy in mine:
        copy.start()
    lax.fori_loop(0, NZ * NY, load_w, 0)

    plane = [(i, j) for i in range(NX) for j in range(NY) if (i, j) != (0, 0)]
    barrier = pltpu.get_barrier_semaphore()
    pl.semaphore_signal(barrier, inc=1, device_id=dev(z, y, x, o), device_id_type=MESH)
    for i, j in plane:
        pl.semaphore_signal(barrier, inc=1, device_id=dev(z, yy(j), xx(i), c), device_id_type=MESH)
    for k in range(1, NZ):
        pl.semaphore_signal(barrier, inc=1, device_id=dev(zz(k), y, x, c), device_id_type=MESH)
    for k in range(1, 4):
        pl.semaphore_signal(barrier, inc=1, device_id=dev(z, yy(k), x, o), device_id_type=MESH)
        pl.semaphore_signal(barrier, inc=1, device_id=dev(z, y, xx(k), o), device_id_type=MESH)
    pl.semaphore_wait(barrier, 1 + len(plane) + NZ - 1 + 6)
    for copy in mine:
        copy.wait()

    count = [0]
    sends = []

    def slot():
        count[0] += 1
        return count[0] - 1

    def send(ref, device, k, to=None, at=None):
        copy = pltpu.make_async_remote_copy(
            src_ref=ref, dst_ref=ref if to is None else to,
            send_sem=send_sem.at[k], recv_sem=recv_sem.at[k if at is None else at],
            device_id=device, device_id_type=MESH,
        )
        copy.start()
        sends.append(copy)

    def arrived(ref, k):
        pltpu.make_async_remote_copy(
            src_ref=ref, dst_ref=ref, send_sem=send_sem.at[0], recv_sem=recv_sem.at[k],
            device_id=dev(z, y, x, o), device_id_type=MESH,
        ).wait_recv()

    passed = [[] for _ in range(NZ)]

    def pass_on(i, view):
        k = slot()
        send(view(c), dev(z, y, x, o), k)
        passed[i].append((view, k))

    first = [(slot(), slot()) for _ in range(3)]
    for j in range(1, 4):
        send(gat.at[0, z, y, x, c], dev(z, yy(j), x, c), first[j - 1][0])
        send(gat.at[1, z, y, x, c], dev(z, y, xx(j), c), first[j - 1][1])
    w_slot = slot()
    pltpu.make_async_copy(wv.at[:, 0:RV, :], wo, load_sem.at[1]).wait()
    send(wo, dev(z, y, x, o), w_slot, wv.at[:, RV : 2 * RV, :])

    class Ring:
        def __init__(self, q, i):
            self.q, self.i, self.z = q, i, zz(NEAR[i])
            self.k = [slot() for _ in range(4)]

        def view(self, step, lo, hi):
            if self.q == 0:
                return lambda core: gat.at[0, self.z, lo:hi, xx(step), core]
            return lambda core: gat.at[1, self.z, yy(step), lo:hi, core]

        def to(self, step):
            return dev(z, y, xx(step), c) if self.q == 0 else dev(z, yy(step), x, c)

        def open(self):
            send(self.view(0, 0, 4)(c), self.to(1), self.k[0])
            send(self.view(0, 0, 4)(c), self.to(-1), self.k[1])

        def middle(self):
            low, high = self.view(-1, 0, 4), self.view(1, 0, 4)
            arrived(low(c), self.k[0])
            send(self.view(-1, 0, 2)(c), self.to(1), self.k[2])
            pass_on(self.i, low)
            arrived(high(c), self.k[1])
            send(self.view(1, 2, 4)(c), self.to(-1), self.k[3])
            pass_on(self.i, high)

        def close(self):
            low, high = self.view(-2, 0, 2), self.view(2, 2, 4)
            arrived(low(c), self.k[2])
            pass_on(self.i, low)
            arrived(high(c), self.k[3])
            pass_on(self.i, high)

    ring = [(Ring(0, i), Ring(1, i)) for i in range(NZ)]

    def opened(*chunks):
        for i in chunks:
            ring[i][0].open()
            ring[i][1].open()

    def middle(i):
        ring[i][0].middle()
        ring[i][1].middle()

    def close(i):
        ring[i][0].close()
        ring[i][1].close()

    def unit(q, z_, lo, hi):
        if q == 0:
            return lambda core: gat.at[0, z_, lo:hi, x, core]
        return lambda core: gat.at[1, z_, y, lo:hi, core]

    near = (0, -1, 1, 2)

    def block(q, z_, m):
        if q == 0:
            return gat.at[0, z_, yy(near[m]), x, c]
        return gat.at[1, z_, y, xx(near[m]), c]

    def far(d, m):
        return (m < 2) == (d == 0)

    k_ring = {
        (d, k, m, q): slot()
        for d in range(2) for k in range(1, 5) for m in range(4) for q in range(2)
        if k < 4 or far(d, m)
    }

    def z_open(m):
        for q in range(2):
            for d in range(2):
                send(block(q, z, m), dev(zz(1 - 2 * d), y, x, c), k_ring[d, 1, m, q])

    def z_block(k, m):
        for q in range(2):
            for d in range(2):
                if k < 4 or far(d, m):
                    ref = block(q, zz(k * (2 * d - 1)), m)
                    arrived(ref, k_ring[d, k, m, q])
                    if k < 3 or (k == 3 and far(d, m)):
                        send(ref, dev(zz(1 - 2 * d), y, x, c), k_ring[d, k + 1, m, q])

    def z_done(*chunks):
        opened(*chunks)
        for i in chunks:
            for q in range(2):
                pass_on(i, unit(q, zz(NEAR[i]), 0, 4))

    def logits_step(i):
        for view, k in passed[i]:
            arrived(view(o), k)
        if i == 0:
            pltpu.make_async_copy(wo, wv.at[:, 0:RV, :], load_sem.at[0]).wait()
        zs = zz(NEAR[i])
        left, right = [], []
        for j in range(NY):
            left += [wv[zs * NY + j, 0:RV], wo[zs * NY + j]]
            right += [gat[c, zs, j].reshape(T, 128), gat[o, zs, j].reshape(T, 128)]
        res = lax.dot_general(
            jnp.concatenate(left, axis=1), jnp.concatenate(right, axis=1),
            (((1,), (1,)), ((), ())), preferred_element_type=F32,
        )
        if i == 0:
            acc[...] = res
        else:
            acc[...] += res

    def first_block(m):
        j = (0, 1, 3, 2)[m]
        arrived(gat.at[0, z, yy(-j), x, c], first[j - 1][0])
        arrived(gat.at[1, z, y, xx(-j), c], first[j - 1][1])
        z_open(m)

    z_open(0)
    first_block(1)
    first_block(2)
    z_block(1, 0)
    first_block(3)
    z_done(0)
    z_block(1, 1)
    z_block(1, 2)
    z_block(2, 0)
    z_block(1, 3)
    z_done(1, 2)
    z_block(2, 1)
    z_block(2, 2)
    z_block(3, 0)
    middle(0)
    z_block(2, 3)
    z_done(3, 4)
    z_block(3, 1)
    z_block(3, 2)
    z_block(4, 0)
    middle(1)
    z_block(3, 3)
    z_done(5, 6)
    middle(2)
    z_block(4, 1)
    z_block(4, 2)
    z_block(4, 3)
    z_done(7)
    middle(3)
    close(0)
    middle(4)
    logits_step(0)
    close(1)
    middle(5)
    close(2)
    logits_step(1)
    middle(6)
    close(3)
    logits_step(2)
    close(4)
    middle(7)
    logits_step(3)
    close(5)
    logits_step(4)
    close(6)
    logits_step(5)
    close(7)
    logits_step(6)
    logits_step(7)
    acc_slot = slot()
    send(acc, dev(z, y, x, o), acc_slot, acc_o)
    arrived(wv.at[:, RV : 2 * RV, :], w_slot)

    offset = (v * (NX * NC) + s) * RV
    picked = tgt[...] - offset == lax.broadcasted_iota(jnp.int32, (RV, T), 0)
    logits = acc[...]
    hit = jnp.sum(jnp.where(picked, logits, 0.0), axis=0, keepdims=True)
    top = jnp.max(logits, axis=0, keepdims=True)
    total = jnp.sum(jnp.exp(logits - top), axis=0, keepdims=True)
    state = jnp.concatenate([packed(top), packed(total), packed(hit), jnp.zeros((4, 128), F32)], axis=0)

    def merged(blocks):
        tops = [block[0:4] for block in blocks]
        top = tops[0]
        for one in tops[1:]:
            top = jnp.maximum(top, one)
        total, hit = jnp.zeros_like(top), jnp.zeros_like(top)
        for block, one in zip(blocks, tops):
            total = total + block[4:8] * jnp.exp(one - top)
            hit = hit + block[8:12]
        return jnp.concatenate([top, total, hit, jnp.zeros((4, 128), F32)], axis=0)

    def exchanged(state, buf, me, n, peers):
        buf[me] = state
        todo = []
        for device, source, k in peers:
            send(buf.at[me], device, k)
            todo.append((source, k))
        for source, k in todo:
            arrived(buf.at[source], k)
        return merged([buf[k] for k in range(n)])

    state = exchanged(state, rx_c, c, 2, [(dev(z, y, x, o), o, slot())])
    state = exchanged(
        state, rx_p, x * NY + y, NX * NY,
        [(dev(z, yy(j), xx(i), c), xx(-i) * NY + yy(-j), slot()) for i, j in plane],
    )
    state = exchanged(
        state, rx_z, z, NZ, [(dev(zz(k), y, x, c), zz(-k), slot()) for k in range(1, NZ)]
    )
    loss[...] = unpacked(state[0:4] + jnp.log(state[4:8]) - state[8:12])
    top, total = unpacked(state[0:4]), unpacked(state[4:8])
    dlt[...] = (jnp.exp(acc[...] - top) / total - picked.astype(F32)).astype(BF16)

    arrived(acc_o, acc_slot)
    offset_o = (v * (NX * NC) + x * NC + o) * RV
    picked_o = tgt[...] - offset_o == lax.broadcasted_iota(jnp.int32, (RV, T), 0)
    dlt_o = (jnp.exp(acc_o[...] - top) / total - picked_o.astype(F32)).astype(BF16)
    for k, value in ((0, dlt[...]), (RV, dlt_o)):
        value = jnp.transpose(value)
        dl[:, k : k + RV] = jnp.concatenate([value[64:T], value[0:64]], axis=0)

    def weight_step(k):
        right = []
        for j in range(NY):
            right += [gat[0, k, j].reshape(T, 128), gat[1, k, j].reshape(T, 128)]
        wg[:, 1024 * k : 1024 * (k + 1)] = jnp.dot(
            dlt[...], jnp.concatenate(right, axis=1), preferred_element_type=F32
        ).astype(BF16)

    def hidden_step(i):
        zd = zz(ORDER[i])
        right = jnp.concatenate([wv[zd * NY + j] for j in range(NY)], axis=1)
        res = jnp.dot(dl[...], right, preferred_element_type=F32)
        for j in range(NY):
            part[i, j] = res[:, 128 * j : 128 * (j + 1)].reshape(NX, 128, 128)

    class Heavy:
        def __init__(self, unit, along, s1, r1, s2, r2):
            self.unit, self.along = unit, along
            self.s1, self.r1, self.s2, self.r2 = s1, r1, s2, r2
            self.k = [[slot() for _ in range(4)] for _ in range(NZ)]

        def to(self, step):
            return dev(z, y, xx(step), c) if self.along == "x" else dev(z, yy(step), x, c)

        def first(self, i):
            self.s1[i] = self.unit(i, 2).astype(WIRE)
            k = self.k[i]
            send(self.s1.at[i, 0:2], self.to(1), k[0], self.r1.at[i, 0:2])
            send(self.s1.at[i, 2:4], self.to(-1), k[1], self.r1.at[i, 2:4])

        def second(self, i):
            k = self.k[i]
            for d, lo, hi in ((0, 0, 2), (1, 2, 4)):
                step = 1 - 2 * d
                arrived(self.r1.at[i, lo:hi], k[d])
                mine = self.unit(i, step)
                self.s2[i, d] = mine.astype(WIRE)
                self.s2[i, d, lo:hi] = (mine[lo:hi] + self.r1[i, lo:hi].astype(F32)).astype(WIRE)
                send(self.s2.at[i, d], self.to(step), k[2 + d], self.r2.at[i, d])

        def third(self, i):
            for d in range(2):
                arrived(self.r2.at[i, d], self.k[i][2 + d])
            return self.unit(i, 0) + self.r2[i, 0].astype(F32) + self.r2[i, 1].astype(F32)

    hb = Heavy(lambda i, step: part[i, :, xx(step), B, :], "x", sb1, rb1, sb2, rb2)
    hc = Heavy(lambda i, step: part[i, yy(step), :, C, :], "y", sc1, rc1, sc2, rc2)

    def thirds(i):
        qs[i, 0] = hb.third(i)
        qs[i, 1] = hc.third(i)

    k_z = {(d, off, h, q): slot() for d in range(2) for off in range(1, 5) for h in range(2) for q in range(2)}

    def z_send(d, off, h):
        i = ORDER.index(off if d == 0 or off == 4 else -off)
        rows = slice(2 * h, 2 * h + 2)
        for q in range(2):
            k, value = k_z[d, off, h, q], qs[i, q, rows]
            if off < 3 or (off == 3 and h == d):
                came = rzb.at[d, 3 - off] if off > 1 else rzf.at[d, 0]
                arrived(came.at[q, rows], k_z[d, off + 1, h, q])
                value = value + came[q, rows].astype(F32)
            if off > 2:
                zb[d, 4 - off, q, rows] = value.astype(WIRE)
                src, dst = zb.at[d, 4 - off, q, rows], rzb.at[d, 4 - off, q, rows]
            else:
                qs[i, q, rows] = value
                src, dst = qs.at[i, q, rows], rzf.at[d, 2 - off, q, rows]
            send(src, dev(zz(1 - 2 * d), y, x, c), k, dst)

    f_send = [[slot() for _ in range(4)] for _ in range(2)]
    f_recv = slot()
    for _ in range(7):
        slot()

    def last_send(q):
        for d in range(2):
            for h in range(2):
                arrived(rzf.at[d, 1, q, 2 * h : 2 * h + 2], k_z[d, 1, h, q])
        fz[q] = qs[NZ - 1, q] + rzf[0, 1, q] + rzf[1, 1, q]
        for j in range(1, 4):
            block = yy(j) if q == 0 else xx(j)
            device = dev(z, block, x, 0) if q == 0 else dev(z, y, block, 1)
            send(fz.at[q, block], device, f_send[q][j], rf.at[c, j], f_recv + 4 * c + j)


    def go(i):
        hidden_step(i)
        hb.first(i)
        hc.first(i)

    def second(i):
        hb.second(i)
        hc.second(i)

    go(0)
    go(1)
    go(2)
    weight_step(0)
    second(0)
    go(3)
    second(1)
    go(4)
    second(2)
    weight_step(1)
    thirds(0)
    z_send(0, 4, 0)
    z_send(1, 4, 1)
    go(5)
    second(3)
    thirds(1)
    z_send(0, 3, 1)
    go(6)
    second(4)
    weight_step(2)
    thirds(2)
    z_send(1, 3, 0)
    z_send(0, 3, 0)
    z_send(1, 3, 1)
    go(7)
    second(5)
    thirds(3)
    z_send(0, 2, 1)
    z_send(0, 2, 0)
    second(6)
    weight_step(3)
    thirds(4)
    z_send(1, 2, 0)
    z_send(1, 2, 1)
    second(7)
    weight_step(4)
    thirds(5)
    z_send(0, 1, 1)
    z_send(0, 1, 0)
    weight_step(5)
    thirds(6)
    z_send(1, 1, 0)
    z_send(1, 1, 1)
    weight_step(6)
    thirds(7)
    weight_step(7)
    last_send(0)
    last_send(1)
    mine = y * (1 - c) + x * c
    theirs = y * (1 - o) + x * o
    send(fz.at[o, theirs], dev(z, y, x, o), f_send[0][0], rf.at[c, 0], f_recv + 4 * c)
    rf[c, 0] = fz[c, mine]
    arrived(rf.at[o, 0], f_recv + 4 * o)
    for core in range(2):
        for j in range(1, 4):
            arrived(rf.at[core, j], f_recv + 4 * core + j)
    for core in range(2):
        total = rf[core, 0] + rf[core, 1] + rf[core, 2] + rf[core, 3]
        sent[:, 128 * core : 128 * (core + 1)] = total.astype(BF16)
    for copy in sends:
        copy.wait_send()
    assert count[0] <= N_SEM, count


def on_device(hidden, targets, out_weight):
    hbm, vmem = pl.BlockSpec(memory_space=pl.ANY), pl.BlockSpec(memory_space=pltpu.VMEM)
    heavy = [
        pltpu.VMEM((NZ, 4, 64, 128), WIRE),
        pltpu.VMEM((NZ, 4, 64, 128), WIRE),
        pltpu.VMEM((NZ, 2, 4, 64, 128), WIRE),
        pltpu.VMEM((NZ, 2, 4, 64, 128), WIRE),
    ]
    loss, weight_grad, sent = pl.pallas_call(
        body,
        out_shape=(
            jax.ShapeDtypeStruct((1, T), F32),
            jax.ShapeDtypeStruct((RV, D), BF16),
            jax.ShapeDtypeStruct((64, 256), BF16),
        ),
        in_specs=[hbm, vmem, hbm],
        out_specs=(vmem, vmem, vmem),
        scratch_shapes=[
            pltpu.VMEM((2, NZ, NY, NX, NC, 64, 128), BF16),
            pltpu.VMEM((NZ * NY, 2 * RV, 128), BF16),
            pltpu.VMEM((NZ * NY, RV, 128), BF16),
            pltpu.VMEM((RV, T), F32),
            pltpu.VMEM((RV, T), F32),
            pltpu.VMEM((RV, T), BF16),
            pltpu.VMEM((NC, 16, 128), F32),
            pltpu.VMEM((NX * NY, 16, 128), F32),
            pltpu.VMEM((NZ, 16, 128), F32),
            pltpu.VMEM((T, 2 * RV), BF16),
            pltpu.VMEM((NZ, NY, NX, 128, 128), F32),
            *heavy,
            *heavy,
            pltpu.VMEM((NZ, 2, 4, 64, 128), F32),
            pltpu.VMEM((2, 2, 2, 4, 64, 128), WIRE),
            pltpu.VMEM((2, 2, 2, 4, 64, 128), WIRE),
            pltpu.VMEM((2, 2, 2, 4, 64, 128), F32),
            pltpu.VMEM((2, 4, 64, 128), F32),
            pltpu.VMEM((2, 4, 64, 128), F32),
            pltpu.SemaphoreType.DMA((N_SEM,)),
            pltpu.SemaphoreType.DMA((N_SEM,)),
            pltpu.SemaphoreType.DMA((2,)),
            pltpu.SemaphoreType.DMA((2,)),
        ],
        compiler_params=pltpu.CompilerParams(
            collective_id=0, has_side_effects=True, vmem_limit_bytes=46 * 2**20
        ),
    )(hidden, targets.reshape(1, T), out_weight)
    return loss.reshape(T), weight_grad, sent


def solution(mesh):
    placed = (P("section", "vocab"), P(), P(("vocab", "section"), None))
    return jax.shard_map(
        on_device, mesh=mesh, in_specs=placed,
        out_specs=(P(), P(("vocab", "section"), None), P("section", "vocab")),
        check_vma=False,
    )
```
